32 devices in a mesh: tm: 8 (over y, x, core), space: 4 (over z).
Axes of the slice: x: 2, y: 2, z: 4, core: 2. Of those that a mesh axis runs over, the one named last changes fastest.
Arguments:
- speed: float32 [8, 16, 128], P('space'), may hold values from 0.5 to 1.5
- forcing: float32 [32, 8, 16, 128], P('tm', 'space'), may hold values from -1.8 to 1.8
- guess: float32 [8, 4, 8, 16, 128], P('tm', None, 'space'), may hold values from -8 to 8
- basis: float32 [8, 64, 4, 8, 16, 128], P('tm', None, None, 'space'), may hold values from -1 to 1, as said below
Outputs:
- states: float32 [32, 4, 8, 16, 128], P('tm', None, 'space')
- coords: float32 [8, 64], P('tm')
The draws below stay inside these ranges and needn't reach their ends.
Inputs may be any that keep to these rules, and one draw needn't show every extreme that they name: The columns of each basis[k] are linearly independent.
All inputs are finite; a program needn't handle non-finite values.
Results may differ from the reference program's by a relative error of at most 0.00018.
Values sent between devices are 32-bit elements; how exact they have to be, the bound alone decides.
A program may use at most 128 MiB of HBM per device.

```python
import jax
import jax.numpy as jnp
from jax import lax

NX = 16
NY = 128
RANK = 64
NZ = 8
NT = 32
N_TM = 8


DT = 0.045


def shifted_ahead_drawn(values, axis):
    size = values.shape[axis]
    rest = lax.slice_in_dim(values, 1, size, axis=axis)
    border = jnp.zeros_like(lax.slice_in_dim(values, 0, 1, axis=axis))
    return jnp.concatenate([rest, border], axis=axis)


def shifted_behind_drawn(values, axis):
    size = values.shape[axis]
    rest = lax.slice_in_dim(values, 0, size - 1, axis=axis)
    border = jnp.zeros_like(lax.slice_in_dim(values, 0, 1, axis=axis))
    return jnp.concatenate([border, rest], axis=axis)


def fine_advance(state, speed_sq):
    pressure = state[..., 0, :, :, :]
    depth = pressure.ndim
    flow_x = state[..., 1, :, :, :] - DT * (shifted_ahead_drawn(pressure, depth - 2) - pressure)
    flow_y = state[..., 2, :, :, :] - DT * (shifted_ahead_drawn(pressure, depth - 1) - pressure)
    flow_z = state[..., 3, :, :, :] - DT * (shifted_ahead_drawn(pressure, depth - 3) - pressure)
    diverge = flow_x - shifted_behind_drawn(flow_x, depth - 2) + (flow_y - shifted_behind_drawn(flow_y, depth - 1)) + (flow_z - shifted_behind_drawn(flow_z, depth - 3))
    fresh = pressure - DT * speed_sq * diverge
    return jnp.stack([fresh, flow_x, flow_y, flow_z], axis=depth - 3)


def speed_field(key):
    log_speed = jax.random.uniform(jax.random.fold_in(key, 202), (NZ, NX, NY), jnp.float32, jnp.log(0.5), jnp.log(1.5))
    return jnp.clip(jnp.exp(log_speed), 0.5, 1.5)


def pattern_block(key, block_index):
    return jax.random.normal(jax.random.fold_in(jax.random.fold_in(key, 101), block_index), (RANK, 4, NZ, NX, NY), jnp.float32)


def draw_speed(key, part):
    return speed_field(key)


def draw_guess(key, part):
    mixing = jax.random.normal(jax.random.fold_in(key, 404), (N_TM, RANK), jnp.float32)

    def aligned(block_index):
        block = pattern_block(key, block_index)
        factors = mixing[block_index][:, None, None, None, None]
        return jnp.sum(factors * block, axis=0) / jnp.sqrt(jnp.float32(RANK))
    aligned_all = lax.map(aligned, jnp.arange(N_TM, dtype=jnp.int32))
    rough_part = jax.random.normal(jax.random.fold_in(key, 303), aligned_all.shape, jnp.float32)
    strength = 1.0
    return jnp.clip(rough_part + strength * aligned_all, -8.0, 8.0)


def draw_basis(key, part):
    speed_sq = jnp.square(speed_field(key))
    cell_count = 4 * NZ * NX * NY
    blend_weight = 0.0
    least_scale = 0.3
    most_scale = 3.0
    scales = jnp.exp(jax.random.uniform(jax.random.fold_in(key, 505), (N_TM, RANK), jnp.float32, jnp.log(least_scale), jnp.log(most_scale)))

    def column_block(block_index):
        source = (block_index + N_TM - 2) % N_TM
        moved_block = pattern_block(key, source)
        for repeat in range(4):
            moved_block = fine_advance(moved_block, speed_sq)
        common = jnp.sum(moved_block, axis=0) / jnp.sqrt(jnp.float32(RANK))
        mixed_columns = moved_block + blend_weight * common[None]
        column_scale = scales[block_index] / jnp.sqrt(jnp.float32(cell_count))
        return mixed_columns * column_scale[:, None, None, None, None]
    columns = lax.map(column_block, jnp.arange(N_TM, dtype=jnp.int32))
    return jnp.clip(columns, -1.0, 1.0)


def steps_of(own_key, extent, cuts, least, largest):
    level = 1.0
    for axis_at, shards_of in cuts:
        draws = jax.random.uniform(jax.random.fold_in(jax.random.fold_in(own_key, 6), axis_at), (shards_of,), jnp.float32, least / len(cuts), largest / len(cuts))
        level = level * jnp.repeat(jnp.exp(draws), extent[axis_at] // shards_of).reshape((-1,) + (1,) * (len(extent) - 1 - axis_at))
    return level


def bell_draw(own_key, shape, scale, most, cuts=(), held_as=jnp.bfloat16):
    drawn = scale * jax.random.normal(own_key, shape, jnp.float32)
    if cuts:
        drawn = drawn * steps_of(own_key, shape, cuts, -0.22, 0.18)
    return jnp.clip(drawn, -most, most).astype(held_as)


def setup_inputs(seed: int = 0) -> dict:
    key_list = jax.random.split(jax.random.key(seed), 5)
    return {
        "speed": draw_speed(jax.random.fold_in(key_list[4], 71), 0),
        "forcing": bell_draw(key_list[1], (NT, NZ, NX, NY), 0.3, 1.8, ((0, 8), (1, 4)), jnp.float32),
        "guess": draw_guess(jax.random.fold_in(key_list[4], 71), 0),
        "basis": draw_basis(jax.random.fold_in(key_list[4], 71), 0),
    }


DT = 0.045
exact_mode = lax.Precision.HIGHEST

def shifted_ahead(values, axis):
    size = values.shape[axis]
    rest = lax.slice_in_dim(values, 1, size, axis=axis)
    border = jnp.zeros_like(lax.slice_in_dim(values, 0, 1, axis=axis))
    return jnp.concatenate([rest, border], axis=axis)

def shifted_behind(values, axis):
    size = values.shape[axis]
    rest = lax.slice_in_dim(values, 0, size - 1, axis=axis)
    border = jnp.zeros_like(lax.slice_in_dim(values, 0, 1, axis=axis))
    return jnp.concatenate([border, rest], axis=axis)

def update_flow(state, upper_plane, delta_time):
    pressure = state[..., 0, :, :, :]
    depth = pressure.ndim
    above = jnp.concatenate([pressure[..., 1:, :, :], upper_plane], axis=depth - 3)
    flow_x = state[..., 1, :, :, :] - delta_time * (shifted_ahead(pressure, depth - 2) - pressure)
    flow_y = state[..., 2, :, :, :] - delta_time * (shifted_ahead(pressure, depth - 1) - pressure)
    flow_z = state[..., 3, :, :, :] - delta_time * (above - pressure)
    return (pressure, flow_x, flow_y, flow_z)

def update_pressure(pressure, flow_x, flow_y, flow_z, lower_plane, speed_sq, delta_time):
    depth = pressure.ndim
    below = jnp.concatenate([lower_plane, flow_z[..., :-1, :, :]], axis=depth - 3)
    diverge = flow_x - shifted_behind(flow_x, depth - 2) + (flow_y - shifted_behind(flow_y, depth - 1)) + (flow_z - below)
    fresh = pressure - delta_time * speed_sq * diverge
    return jnp.stack([fresh, flow_x, flow_y, flow_z], axis=depth - 3)

def advance(state, speed_sq, delta_time):
    zero_plane = jnp.zeros_like(state[..., 0, :1, :, :])
    pressure, flow_x, flow_y, flow_z = update_flow(state, zero_plane, delta_time)
    return update_pressure(pressure, flow_x, flow_y, flow_z, zero_plane, speed_sq, delta_time)

def solve_gram(chol, coef):
    lifted = lax.linalg.triangular_solve(chol, coef[..., None], left_side=True, lower=True)
    solved = lax.linalg.triangular_solve(chol, lifted, left_side=True, lower=True, transpose_a=True)
    return solved[..., 0]

def reference(speed, forcing, guess, basis):
    count = guess.shape[0]
    speed_sq = speed * speed
    loads = forcing.reshape(count, 4, forcing.shape[1], forcing.shape[2], forcing.shape[3])

    def fine_step(state, row_index):
        moved = advance(state, speed_sq, DT)
        return moved.at[:, 0].add(loads[:, row_index])

    def sweep(left):
        points = []
        current = left
        for row_index in range(3):
            current = fine_step(current, row_index)
            points.append(current)
        return points

    def from_left(values):
        return jnp.roll(values, 1, axis=0)
    first_points = sweep(from_left(guess))
    relaxed = fine_step(first_points[-1], 3)
    second_points = sweep(from_left(relaxed))
    residue = fine_step(second_points[-1], 3) - relaxed
    flat_basis = basis.reshape(count, basis.shape[1], -1)

    def build(columns):
        moved = columns
        for repeat in range(4):
            moved = advance(moved, speed_sq, DT)
        return (moved - advance(columns, speed_sq, 4 * DT)).reshape(columns.shape[0], -1)
    corrections = lax.map(build, basis)
    gram = jnp.einsum('krn,ksn->krs', flat_basis, flat_basis, precision=exact_mode)
    chol = jnp.linalg.cholesky(gram)

    def candidate(levels):
        left = from_left(levels)
        moved = advance(left, speed_sq, 4 * DT)
        coef = jnp.einsum('krn,kn->kr', flat_basis, left.reshape(count, -1), precision=exact_mode)
        weights = solve_gram(chol, coef)
        extra = jnp.einsum('kr,krn->kn', weights, corrections, precision=exact_mode).reshape(left.shape)
        return moved + extra + residue
    levels = candidate(residue)
    levels = candidate(levels)
    gap = candidate(levels) - levels
    carry = gap[0:4]
    chained = [carry]
    for group in range(1, count // 4):
        carry = advance(advance(carry, speed_sq, 8 * DT), speed_sq, 8 * DT) + gap[4 * group:4 * group + 4]
        chained.append(carry)
    chain = jnp.concatenate(chained, axis=0)
    levels = candidate(levels + chain)
    final_c = relaxed + levels
    third_points = sweep(from_left(final_c))
    states = jnp.stack(third_points + [final_c], axis=1)
    states = states.reshape(count * 4, 4, guess.shape[2], guess.shape[3], guess.shape[4])
    coef = jnp.einsum('krn,kn->kr', flat_basis, final_c.reshape(count, -1), precision=exact_mode)
    coords = solve_gram(chol, coef)
    return (states, coords)
```

```python
import jax
import jax.numpy as jnp
from jax import lax
from jax.experimental import pallas as pl
from jax.experimental.pallas import tpu as pltpu
from jax.sharding import PartitionSpec as P

DT = 0.045
GROUP = 4
MESH = pl.DeviceIdType.MESH


def phi(state, speed_sq, h):
    p, vx, vy, vz = state
    nx, ny = p.shape[1], p.shape[2]
    row = lax.broadcasted_iota(jnp.int32, p.shape, 1)
    lane = lax.broadcasted_iota(jnp.int32, p.shape, 2)
    zero = jnp.zeros_like(p[:1])
    px = jnp.where(row == nx - 1, 0.0, pltpu.roll(p, nx - 1, 1))
    py = jnp.where(lane == ny - 1, 0.0, pltpu.roll(p, ny - 1, 2))
    pz = jnp.concatenate([p[1:], zero], axis=0)
    vx = vx - h * (px - p)
    vy = vy - h * (py - p)
    vz = vz - h * (pz - p)
    bx = jnp.where(row == 0, 0.0, pltpu.roll(vx, 1, 1))
    by = jnp.where(lane == 0, 0.0, pltpu.roll(vy, 1, 2))
    bz = jnp.concatenate([zero, vz[:-1]], axis=0)
    p = p - h * speed_sq * ((vx - bx) + (vy - by) + (vz - bz))
    return (p, vx, vy, vz)


def make_kernel(n_tm, n_sp, rank, slab):
    n_chain = n_tm // GROUP - 1

    def kernel(
        speed_in, forcing_in, guess_in, basis_in, states_out, coords_out,
        speed, forcing, basis, rx, tx, ys, cf, gb, inv, acc, wb,
        local_sem, in_s, in_r, sh_s, sh_r, y_s, y_r, c_s, c_r, g_s, g_r,
    ):
        k = lax.axis_index("tm")
        s = lax.axis_index("space")
        nxt = lax.rem(k + 1, n_tm)
        mine = pl.ds(slab * s, slab)

        def peer(d):
            return lax.rem(s + d, n_sp)

        copies = [
            pltpu.make_async_copy(speed_in, speed.at[mine], local_sem.at[1]),
            pltpu.make_async_copy(forcing_in, forcing.at[:, mine], local_sem.at[2]),
            pltpu.make_async_copy(basis_in, basis, local_sem.at[3]),
        ]
        for c in copies:
            c.start()

        partners = [(k, peer(d)) for d in range(1, n_sp)]
        for d in range(n_sp):
            partners.append((nxt, peer(d)))
            partners.append((lax.rem(k + n_tm - 1, n_tm), peer(d)))
        for j in range(1, n_chain + 1):
            partners.append((lax.rem(k + 1 + GROUP * j, n_tm), s))
            partners.append((lax.rem(k + n_tm - 1 - GROUP * j, n_tm), s))
        barrier = pltpu.get_barrier_semaphore()
        for target in partners:
            pl.semaphore_signal(barrier, inc=1, device_id=target, device_id_type=MESH)
        pl.semaphore_wait(barrier, len(partners))

        def remote(src, dst, send, recv, target):
            c = pltpu.make_async_remote_copy(
                src_ref=src, dst_ref=dst, send_sem=send, recv_sem=recv,
                device_id=target, device_id_type=MESH,
            )
            c.start()
            return c

        sent = []
        first = []
        for d in range(n_sp):
            first.append(remote(guess_in, rx.at[0, :, mine], in_s.at[0, d], in_r.at[0, d], (nxt, peer(d))))
        for d in range(1, n_sp):
            first.append(remote(speed_in, speed.at[mine], in_s.at[1, d], in_r.at[1, d], (k, peer(d))))
            first.append(remote(forcing_in, forcing.at[:, mine], in_s.at[2, d], in_r.at[2, d], (k, peer(d))))
        sent += first

        def load(ref):
            return tuple(ref[i] for i in range(4))

        def store(ref, state):
            for i in range(4):
                ref[i] = state[i]

        def fine(i, state):
            p, vx, vy, vz = phi(state, speed[...] * speed[...], DT)
            return (p + forcing[i], vx, vy, vz)

        def plain(i, state):
            return phi(state, speed[...] * speed[...], DT)

        def shift_whole(index, src, hop):
            c = remote(src, rx.at[index], sh_s.at[index, 0], sh_r.at[index, 0], (lax.rem(k + hop, n_tm), s))
            sent.append(c)
            return c

        def shift_slabs(index, src):
            made = []
            for d in range(n_sp):
                part = pl.ds(slab * peer(d), slab)
                made.append(remote(src.at[:, part], rx.at[index, :, part], sh_s.at[index, d], sh_r.at[index, d], (nxt, s)))
            sent.extend(made)
            return made

        copies[2].wait()

        def gram_step(i, total):
            t = jnp.swapaxes(basis[:, i], 0, 1)
            hi = t.astype(jnp.bfloat16)
            rest = t - hi.astype(jnp.float32)
            mid = rest.astype(jnp.bfloat16)
            low = (rest - mid.astype(jnp.float32)).astype(jnp.bfloat16)
            parts = jnp.concatenate([hi, mid, low], axis=1)
            flat = jnp.concatenate([parts[j] for j in range(parts.shape[0])], axis=1)
            return total + lax.dot_general(
                flat, flat, (((1,), (1,)), ((), ())), preferred_element_type=jnp.float32
            )

        full = lax.fori_loop(0, basis.shape[1], gram_step, jnp.zeros((3 * rank, 3 * rank), jnp.float32))
        hh, hm, hl = full[:rank, :rank], full[:rank, rank:2 * rank], full[:rank, 2 * rank:]
        mh, mm, lh = full[rank:2 * rank, :rank], full[rank:2 * rank, rank:2 * rank], full[2 * rank:, :rank]
        gram = hh + ((hm + mh) + (mm + (hl + lh)))
        gb[s] = jnp.concatenate([gram, jnp.zeros_like(gram)], axis=1)
        gram_copies = [remote(gb.at[s], gb.at[s], g_s.at[d], g_r.at[d], (k, peer(d))) for d in range(1, n_sp)]
        sent += gram_copies

        copies[0].wait()
        copies[1].wait()
        for c in first:
            c.wait_recv()
        state = lax.fori_loop(0, 4, fine, load(rx.at[0]))
        store(tx.at[0], state)
        moved = shift_whole(1, tx.at[0], 1)

        for c in gram_copies:
            c.wait_recv()
        g = gb[0]
        for i in range(1, n_sp):
            g = g + gb[i]
        rows = lax.broadcasted_iota(jnp.int32, g.shape, 0)
        lanes = lax.broadcasted_iota(jnp.int32, g.shape, 1)
        m = jnp.where(lanes == rows + rank, 1.0, g)
        for j in range(rank):
            pivot = m[j:j + 1]
            pivot = pivot / pivot[:, j:j + 1]
            m = jnp.where(rows == j, pivot, m - m[:, j:j + 1] * pivot)
        inverse = m[:, rank:]
        inv[...] = jnp.concatenate([inverse, jnp.zeros_like(inverse)], axis=1)
        acc[rank:, :] = jnp.zeros((rank, acc.shape[1]), jnp.float32)

        moved.wait_recv()
        state = lax.fori_loop(0, 4, fine, load(rx.at[1]))
        residue = tx.at[1]
        for i in range(4):
            residue[i] = state[i] - tx[0, i]

        def weights(index, x):
            def coef_step(i, carry):
                b = basis[pl.ds(8 * i, 8)]
                t = jnp.sum(b * x[None], axis=1)
                half = t.shape[1] // 2
                t = t[:, :half] + t[:, half:]
                acc[pl.ds(pl.multiple_of(8 * i, 8), 8), :] = jnp.sum(t, axis=1)
                return carry

            lax.fori_loop(0, rank // 8, coef_step, 0)
            ones = jnp.ones((8, acc.shape[1]), jnp.float32)
            cf[index, s] = lax.dot_general(
                ones, acc[...], (((1,), (1,)), ((), ())),
                precision=lax.Precision.HIGHEST, preferred_element_type=jnp.float32,
            )
            made = [
                remote(cf.at[index, s], cf.at[index, s], c_s.at[index, d], c_r.at[index, d], (k, peer(d)))
                for d in range(1, n_sp)
            ]
            sent.extend(made)
            return made

        def solve(index, made):
            for c in made:
                c.wait_recv()
            total = cf[index, 0]
            for i in range(1, n_sp):
                total = total + cf[index, i]
            w = jnp.sum(inv[...] * total[:1], axis=1, keepdims=True)
            return jnp.broadcast_to(w, wb.shape)

        def slab_of(ref):
            x = ref[:, mine]
            return x.reshape((x.shape[0] * x.shape[1],) + x.shape[2:])

        def candidate(index, x_ref, late):
            wb[...] = solve(index, weights(index, slab_of(x_ref)))

            def sum_step(r, y):
                return y + wb[pl.ds(r, 1), :][None] * basis[r]

            y = lax.fori_loop(0, rank, sum_step, jnp.zeros(basis.shape[1:], jnp.float32), unroll=4)
            ys[index, :, mine] = y.reshape((4, slab) + y.shape[1:])
            made = [
                remote(ys.at[index, :, mine], ys.at[index, :, mine], y_s.at[index, d], y_r.at[index, d], (k, peer(d)))
                for d in range(1, n_sp)
            ]
            sent.extend(made)
            for c in late + made:
                c.wait_recv()
            ally = load(ys.at[index])
            ahead = phi(tuple(x_ref[i] - ally[i] for i in range(4)), speed[...] * speed[...], 4 * DT)
            for i in range(4):
                acc4[i] = ahead[i] + residue[i]
            corrected = lax.fori_loop(0, 4, plain, load(ys.at[index]))
            return tuple(corrected[i] + acc4[i] for i in range(4))

        acc4 = tx.at[6]

        moved = shift_slabs(2, residue)
        for index in range(3):
            moved[0].wait_recv()
            level = candidate(index, rx.at[2 + index], moved[1:])
            store(tx.at[2 + index], level)
            if index < 2:
                moved = shift_slabs(3 + index, tx.at[2 + index])
        for i in range(4):
            tx[5, i] = tx[4, i] - tx[3, i]
        chains = [shift_whole(6 + j, tx.at[5], 1 + GROUP * j) for j in range(1, n_chain + 1)]
        moved = shift_whole(5, tx.at[4], 1)
        source = lax.rem(k + n_tm - 1, n_tm)
        carry = None
        for j in range(n_chain, 0, -1):
            chains[j - 1].wait_recv()
            keep = (source >= GROUP * j).astype(jnp.float32)
            gap = tuple(keep * rx[6 + j, i] for i in range(4))
            carry = gap if carry is None else tuple(a + b for a, b in zip(gap, carry))
            carry = lax.fori_loop(0, 2, lambda i, u: phi(u, speed[...] * speed[...], 8 * DT), carry)
        moved.wait_recv()
        x_ref = rx.at[5]
        if carry is not None:
            for i in range(4):
                ys[4, i] = rx[5, i] + carry[i]
            x_ref = ys.at[4]
        level = candidate(3, x_ref, [])
        final = tx.at[7]
        for i in range(4):
            final[i] = tx[0, i] + level[i]
        moved = shift_whole(6, final, 1)
        made = weights(4, slab_of(final))
        states_out[3] = final[:, mine]
        w = solve(4, made)
        rows = lax.broadcasted_iota(jnp.int32, w.shape, 0)
        lanes = lax.broadcasted_iota(jnp.int32, w.shape, 1)
        coords_out[...] = jnp.sum(jnp.where(rows == lanes, w, 0.0), axis=0, keepdims=True)[:, :rank]
        moved.wait_recv()
        state = load(rx.at[6])
        for n in range(3):
            state = fine(n, state)
            store(acc4, state)
            states_out[n] = acc4[:, mine]
        for c in sent:
            c.wait_send()

    return kernel


def solution(mesh):
    n_tm, n_sp = mesh.shape["tm"], mesh.shape["space"]

    def body(speed, forcing, guess, basis):
        rank = basis.shape[1]
        slab, nx, ny = speed.shape
        nz = slab * n_sp
        n_chain = n_tm // GROUP - 1
        f32 = jnp.float32
        dma = pltpu.SemaphoreType.DMA
        return pl.pallas_call(
            make_kernel(n_tm, n_sp, rank, slab),
            out_shape=(
                jax.ShapeDtypeStruct((4, 4, slab, nx, ny), f32),
                jax.ShapeDtypeStruct((1, rank), f32),
            ),
            in_specs=[pl.BlockSpec(memory_space=pl.ANY)] * 4,
            out_specs=(pl.BlockSpec(memory_space=pltpu.VMEM),) * 2,
            scratch_shapes=[
                pltpu.VMEM((nz, nx, ny), f32),
                pltpu.VMEM((4, nz, nx, ny), f32),
                pltpu.VMEM((rank, 4 * slab, nx, ny), f32),
                pltpu.VMEM((7 + n_chain, 4, nz, nx, ny), f32),
                pltpu.VMEM((8, 4, nz, nx, ny), f32),
                pltpu.VMEM((5, 4, nz, nx, ny), f32),
                pltpu.VMEM((5, n_sp, 8, 2 * rank), f32),
                pltpu.VMEM((n_sp, rank, 2 * rank), f32),
                pltpu.VMEM((rank, 2 * rank), f32),
                pltpu.VMEM((2 * rank, ny), f32),
                pltpu.VMEM((rank, ny), f32),
                dma((4,)),
                dma((3, n_sp)), dma((3, n_sp)),
                dma((7 + n_chain, n_sp)), dma((7 + n_chain, n_sp)),
                dma((4, n_sp)), dma((4, n_sp)),
                dma((5, n_sp)), dma((5, n_sp)),
                dma((n_sp,)), dma((n_sp,)),
            ],
            compiler_params=pltpu.CompilerParams(
                collective_id=0, has_side_effects=True, vmem_limit_bytes=48 * 1024 * 1024
            ),
        )(speed, forcing, guess[0], basis[0].reshape(rank, 4 * slab, nx, ny))

    placed = (
        P("space", None, None),
        P("tm", "space", None, None),
        P("tm", None, "space", None, None),
        P("tm", None, None, "space", None, None),
    )
    return jax.shard_map(
        body,
        mesh=mesh,
        in_specs=placed,
        out_specs=(P("tm", None, "space", None, None), P("tm", None)),
        check_vma=False,
    )
```

```python
import jax
import jax.numpy as jnp
from jax import lax
from jax.experimental import pallas as pl
from jax.experimental.pallas import tpu as pltpu
from jax.sharding import PartitionSpec as P

DT = 0.045
GROUP = 4
MESH = pl.DeviceIdType.MESH


def phi(state, speed_sq, h):
    p, vx, vy, vz = state
    nx, ny = p.shape[1], p.shape[2]
    row = lax.broadcasted_iota(jnp.int32, p.shape, 1)
    lane = lax.broadcasted_iota(jnp.int32, p.shape, 2)
    zero = jnp.zeros_like(p[:1])
    px = jnp.where(row == nx - 1, 0.0, pltpu.roll(p, nx - 1, 1))
    py = jnp.where(lane == ny - 1, 0.0, pltpu.roll(p, ny - 1, 2))
    pz = jnp.concatenate([p[1:], zero], axis=0)
    vx = vx - h * (px - p)
    vy = vy - h * (py - p)
    vz = vz - h * (pz - p)
    bx = jnp.where(row == 0, 0.0, pltpu.roll(vx, 1, 1))
    by = jnp.where(lane == 0, 0.0, pltpu.roll(vy, 1, 2))
    bz = jnp.concatenate([zero, vz[:-1]], axis=0)
    p = p - h * speed_sq * ((vx - bx) + (vy - by) + (vz - bz))
    return (p, vx, vy, vz)


def make_kernel(n_tm, n_sp, rank, slab):
    n_chain = n_tm // GROUP - 1

    def kernel(
        speed_in, forcing_in, guess_in, basis_in, states_out, coords_out,
        speed, forcing, basis, rx, tx, ys, cf, gb, inv, acc, wb,
        local_sem, send_sems, recv_sems,
    ):
        k = lax.axis_index("tm")
        s = lax.axis_index("space")
        nxt = lax.rem(k + 1, n_tm)
        mine = pl.ds(slab * s, slab)

        def peer(d):
            return lax.rem(s + d, n_sp)

        copies = [
            pltpu.make_async_copy(speed_in, speed.at[:, mine], local_sem.at[1]),
            pltpu.make_async_copy(forcing_in, forcing.at[:, mine], local_sem.at[2]),
            pltpu.make_async_copy(basis_in, basis, local_sem.at[3]),
        ]
        for c in copies:
            c.start()

        before = lax.rem(k + n_tm - 1, n_tm)
        partners = [(k, peer(d)) for d in range(1, n_sp)]
        groups = [nxt, before]
        for j in range(1, n_chain + 1):
            groups.append(lax.rem(k + 1 + GROUP * j, n_tm))
            groups.append(lax.rem(k + n_tm - 1 - GROUP * j, n_tm))
        for group in groups:
            partners += [(group, peer(d)) for d in range(n_sp)]
        barrier = pltpu.get_barrier_semaphore()
        for target in partners:
            pl.semaphore_signal(barrier, inc=1, device_id=target, device_id_type=MESH)
        pl.semaphore_wait(barrier, len(partners))

        sent = []

        class Remote:
            def __init__(self, src, dst, target, sends=None, receives=None):
                i = len(sent)
                self.copy = pltpu.make_async_remote_copy(
                    src_ref=src, dst_ref=dst, send_sem=send_sems.at[i], recv_sem=recv_sems.at[i],
                    device_id=target, device_id_type=MESH,
                )
                self.sends, self.receives = sends, receives
                sent.append(self)
                self.under(sends, self.copy.start)

            def under(self, condition, act):
                if condition is None:
                    act()
                else:
                    pl.when(condition)(act)

            def wait_recv(self):
                self.under(self.receives, self.copy.wait_recv)

            def wait_send(self):
                self.under(self.sends, self.copy.wait_send)

        def remote(src, dst, target):
            return Remote(src, dst, target)

        def inside(at):
            return (at >= 0) & (at < n_sp)

        def spread(src, base, dst, group, pieces):
            made = []
            for delta, comps, offset, planes in pieces:
                made.append(Remote(
                    src.at[comps, pl.ds(base + offset, planes)],
                    dst.at[comps, pl.ds(slab * s + offset, planes)],
                    (group, s + delta),
                    None if delta == 0 else inside(s + delta),
                    None if delta == 0 else inside(s - delta),
                ))
            return made

        def state_pieces(reach):
            pieces = []
            delta = 1
            while reach - (delta - 1) * slab > 0:
                left = reach - (delta - 1) * slab
                near = min(slab, left - 1)
                if near:
                    pieces.append((delta, slice(0, 4), slab - near, near))
                    pieces.append((-delta, slice(0, 4), 0, near))
                if left <= slab:
                    pieces.append((delta, slice(0, 1), slab - left, 1))
                    pieces.append((delta, slice(3, 4), slab - left, 1))
                    pieces.append((-delta, slice(0, 1), left - 1, 1))
                delta += 1
            return pieces

        own = [(0, slice(0, 4), 0, slab)]

        def load_pieces(reach):
            pieces = []
            delta = 1
            while reach - (delta - 1) * slab > 0:
                left = reach - (delta - 1) * slab
                planes = min(slab, left)
                pieces.append((delta, slice(0, left), slab - planes, planes))
                pieces.append((-delta, slice(0, left), 0, planes))
                delta += 1
            return pieces

        first = spread(guess_in, 0, rx.at[0], nxt, own + state_pieces(4))
        first += spread(forcing_in, 0, forcing, k, load_pieces(3))
        first += spread(speed_in, 0, speed, k, [(d, slice(0, 1), o, n) for d, c, o, n in load_pieces(3)])

        def load(ref):
            return tuple(ref[i] for i in range(4))

        def store(ref, state):
            for i in range(4):
                ref[i] = state[i]

        def fine(i, state):
            p, vx, vy, vz = phi(state, speed[0] * speed[0], DT)
            return (p + forcing[i], vx, vy, vz)

        def plain(i, state):
            return phi(state, speed[0] * speed[0], DT)

        def shift(index, src, group, reach):
            return spread(src, slab * s, rx.at[index], group, own + state_pieces(reach))

        copies[2].wait()

        def gram_step(i, total):
            t = jnp.swapaxes(basis[:, i], 0, 1)
            hi = t.astype(jnp.bfloat16)
            rest = t - hi.astype(jnp.float32)
            mid = rest.astype(jnp.bfloat16)
            low = (rest - mid.astype(jnp.float32)).astype(jnp.bfloat16)
            parts = jnp.concatenate([hi, mid, low], axis=1)
            flat = jnp.concatenate([parts[j] for j in range(parts.shape[0])], axis=1)
            return total + lax.dot_general(
                flat, flat, (((1,), (1,)), ((), ())), preferred_element_type=jnp.float32
            )

        full = lax.fori_loop(0, basis.shape[1], gram_step, jnp.zeros((3 * rank, 3 * rank), jnp.float32))
        hh, hm, hl = full[:rank, :rank], full[:rank, rank:2 * rank], full[:rank, 2 * rank:]
        mh, mm, lh = full[rank:2 * rank, :rank], full[rank:2 * rank, rank:2 * rank], full[2 * rank:, :rank]
        gram = hh + ((hm + mh) + (mm + (hl + lh)))
        gb[s] = jnp.concatenate([gram, jnp.zeros_like(gram)], axis=1)
        gram_copies = [remote(gb.at[s], gb.at[s], (k, peer(d))) for d in range(1, n_sp)]

        copies[0].wait()
        copies[1].wait()
        for c in first:
            c.wait_recv()
        state = lax.fori_loop(0, 4, fine, load(rx.at[0]))
        store(tx.at[0], state)
        moved = shift(1, tx.at[0], nxt, 4)

        for c in gram_copies:
            c.wait_recv()
        g = gb[0]
        for i in range(1, n_sp):
            g = g + gb[i]
        rows = lax.broadcasted_iota(jnp.int32, g.shape, 0)
        lanes = lax.broadcasted_iota(jnp.int32, g.shape, 1)
        m = jnp.where(lanes == rows + rank, 1.0, g)
        for j in range(rank):
            pivot = m[j:j + 1]
            pivot = pivot / pivot[:, j:j + 1]
            m = jnp.where(rows == j, pivot, m - m[:, j:j + 1] * pivot)
        inverse = m[:, rank:]
        inv[...] = jnp.concatenate([inverse, jnp.zeros_like(inverse)], axis=1)
        acc[rank:, :] = jnp.zeros((rank, acc.shape[1]), jnp.float32)

        for c in moved:
            c.wait_recv()
        state = lax.fori_loop(0, 4, fine, load(rx.at[1]))
        residue = tx.at[1]
        for i in range(4):
            residue[i] = state[i] - tx[0, i]

        def weights(index, x):
            def coef_step(i, carry):
                b = basis[pl.ds(8 * i, 8)]
                t = jnp.sum(b * x[None], axis=1)
                half = t.shape[1] // 2
                t = t[:, :half] + t[:, half:]
                acc[pl.ds(pl.multiple_of(8 * i, 8), 8), :] = jnp.sum(t, axis=1)
                return carry

            lax.fori_loop(0, rank // 8, coef_step, 0)
            ones = jnp.ones((8, acc.shape[1]), jnp.float32)
            cf[index, s] = lax.dot_general(
                ones, acc[...], (((1,), (1,)), ((), ())),
                precision=lax.Precision.HIGHEST, preferred_element_type=jnp.float32,
            )
            made = [
                remote(cf.at[index, s], cf.at[index, s], (k, peer(d)))
                for d in range(1, n_sp)
            ]
            return made

        def solve(index, made):
            for c in made:
                c.wait_recv()
            total = cf[index, 0]
            for i in range(1, n_sp):
                total = total + cf[index, i]
            w = jnp.sum(inv[...] * total[:1], axis=1, keepdims=True)
            return jnp.broadcast_to(w, wb.shape)

        def slab_of(ref):
            x = ref[:, mine]
            return x.reshape((x.shape[0] * x.shape[1],) + x.shape[2:])

        def candidate(index, x_ref, late):
            wb[...] = solve(index, weights(index, slab_of(x_ref)))

            def sum_step(r, y):
                return y + wb[pl.ds(r, 1), :][None] * basis[r]

            y = lax.fori_loop(0, rank, sum_step, jnp.zeros(basis.shape[1:], jnp.float32), unroll=4)
            ys[index, :, mine] = y.reshape((4, slab) + y.shape[1:])
            made = spread(ys.at[index], slab * s, ys.at[index], k, state_pieces(4))
            for c in late + made:
                c.wait_recv()
            ally = load(ys.at[index])
            ahead = phi(tuple(x_ref[i] - ally[i] for i in range(4)), speed[0] * speed[0], 4 * DT)
            for i in range(4):
                acc4[i] = ahead[i] + residue[i]
            corrected = lax.fori_loop(0, 4, plain, load(ys.at[index]))
            return tuple(corrected[i] + acc4[i] for i in range(4))

        acc4 = tx.at[6]

        moved = shift(2, residue, nxt, 1)
        for index in range(3):
            moved[0].wait_recv()
            level = candidate(index, rx.at[2 + index], moved[1:])
            store(tx.at[2 + index], level)
            if index < 2:
                moved = shift(3 + index, tx.at[2 + index], nxt, 1)
        for i in range(4):
            tx[5, i] = tx[4, i] - tx[3, i]
        chains = [shift(6 + j, tx.at[5], lax.rem(k + 1 + GROUP * j, n_tm), 2 * j + 1) for j in range(1, n_chain + 1)]
        moved = shift(5, tx.at[4], nxt, 1)
        carry = None
        for j in range(n_chain, 0, -1):
            for c in chains[j - 1]:
                c.wait_recv()
            gap = tuple(jnp.where(before >= GROUP * j, rx[6 + j, i], 0.0) for i in range(4))
            carry = gap if carry is None else tuple(a + b for a, b in zip(gap, carry))
            carry = lax.fori_loop(0, 2, lambda i, u: phi(u, speed[0] * speed[0], 8 * DT), carry)
        for c in moved:
            c.wait_recv()
        x_ref = rx.at[5]
        if carry is not None:
            for i in range(4):
                ys[4, i] = rx[5, i] + carry[i]
            x_ref = ys.at[4]
        level = candidate(3, x_ref, [])
        final = tx.at[7]
        for i in range(4):
            final[i] = tx[0, i] + level[i]
        moved = shift(6, final, nxt, 3)
        made = weights(4, slab_of(final))
        states_out[3] = final[:, mine]
        w = solve(4, made)
        rows = lax.broadcasted_iota(jnp.int32, w.shape, 0)
        lanes = lax.broadcasted_iota(jnp.int32, w.shape, 1)
        coords_out[...] = jnp.sum(jnp.where(rows == lanes, w, 0.0), axis=0, keepdims=True)[:, :rank]
        for c in moved:
            c.wait_recv()
        state = load(rx.at[6])
        for n in range(3):
            state = fine(n, state)
            store(acc4, state)
            states_out[n] = acc4[:, mine]
        for c in sent:
            c.wait_send()

    return kernel


def solution(mesh):
    n_tm, n_sp = mesh.shape["tm"], mesh.shape["space"]

    def body(speed, forcing, guess, basis):
        rank = basis.shape[1]
        slab, nx, ny = speed.shape
        nz = slab * n_sp
        n_chain = n_tm // GROUP - 1
        f32 = jnp.float32
        dma = pltpu.SemaphoreType.DMA
        return pl.pallas_call(
            make_kernel(n_tm, n_sp, rank, slab),
            out_shape=(
                jax.ShapeDtypeStruct((4, 4, slab, nx, ny), f32),
                jax.ShapeDtypeStruct((1, rank), f32),
            ),
            in_specs=[pl.BlockSpec(memory_space=pl.ANY)] * 4,
            out_specs=(pl.BlockSpec(memory_space=pltpu.VMEM),) * 2,
            scratch_shapes=[
                pltpu.VMEM((1, nz, nx, ny), f32),
                pltpu.VMEM((4, nz, nx, ny), f32),
                pltpu.VMEM((rank, 4 * slab, nx, ny), f32),
                pltpu.VMEM((7 + n_chain, 4, nz, nx, ny), f32),
                pltpu.VMEM((8, 4, nz, nx, ny), f32),
                pltpu.VMEM((5, 4, nz, nx, ny), f32),
                pltpu.VMEM((5, n_sp, 8, 2 * rank), f32),
                pltpu.VMEM((n_sp, rank, 2 * rank), f32),
                pltpu.VMEM((rank, 2 * rank), f32),
                pltpu.VMEM((2 * rank, ny), f32),
                pltpu.VMEM((rank, ny), f32),
                dma((4,)),
                dma((128 + 6 * n_sp,)), dma((128 + 6 * n_sp,)),
            ],
            compiler_params=pltpu.CompilerParams(
                collective_id=0, has_side_effects=True, vmem_limit_bytes=60 * 1024 * 1024
            ),
        )(speed[None], forcing, guess[0], basis[0].reshape(rank, 4 * slab, nx, ny))

    placed = (
        P("space", None, None),
        P("tm", "space", None, None),
        P("tm", None, "space", None, None),
        P("tm", None, None, "space", None, None),
    )
    return jax.shard_map(
        body,
        mesh=mesh,
        in_specs=placed,
        out_specs=(P("tm", None, "space", None, None), P("tm", None)),
        check_vma=False,
    )
```
